256 devices in a mesh: frag: 2 (over y), gx: 128 (over x, z, core).
Axes of the slice: x: 4, y: 2, z: 16, core: 2. Of those that a mesh axis runs over, the one named last changes fastest.
The devices are a block of a 4x16x16 slice.
Arguments:
- coefficient: float32 [131072], P(('frag', 'gx')), parts along dimension 0, may hold values from 0.05 to 0.3
- exponent: float32 [131072], P(('frag', 'gx')), parts along dimension 0, may hold values from 0.05 to 0.5
- centers: float32 [3, 131072], P(None, ('frag', 'gx')), parts along dimension 1, may hold values from -2 to 2
- density: float32 [131072], P(('frag', 'gx')), parts along dimension 0, may hold values from -6 to 6
- core_fock: float32 [131072], P(('frag', 'gx')), parts along dimension 0, may hold values from -6 to 6
- shell_ang: int32 [512], P('frag'), parts along dimension 0, may hold values from 0 to 3, as said below
- tile_list: int32 [2, 32768], P(None, ('frag', 'gx')), parts along dimension 1, may hold values from 0 to 255, as said below
Outputs:
- fock: float32 [131072], P(('frag', 'gx')), parts along dimension 0
The draws below stay inside these ranges and needn't reach their ends.
There are 2 independent parts, one for each index of `frag`. The reference program is written for one: setup_inputs(seed, part) draws one part's arguments, and reference() takes and returns one part's arrays. A program takes and returns all parts, laid end to end along the dimension named above; each array names one. Nothing has to cross between parts.
Inputs may be any that keep to these rules, and one draw needn't show every extreme that they name: `shell_ang`: each of 0 to 3 is the angular momentum of exactly 64 blocks; blocks 0 to 1 all have 0. `tile_list`: kind never falls along the list, and kinds 0 to 6 fill 1, 2, 3, 4, 3, 2, 1 sixteenths of the list in turn; pair block b is owned by index b // 2 of gx; among the 128 tiles of one index of gx at most 4 have bra blocks of one owner, and index 0 of gx holds exactly 4 tiles for owner 0.
All inputs are finite; a program needn't handle non-finite values.
Results may differ from the reference program's by a relative error of at most 0.0003.
Values sent between devices are 32-bit elements; how exact they have to be, the bound alone decides.
A program may use at most 128 MiB of HBM per device.

```python
import math
import jax
import jax.numpy as jnp
from jax import lax

PB = 256
MAXL = 3
BLK_DEV = 2
TILE_DEV = 128
NBLK = 256
NPAIR = 65536
NTILE = 16384


def shared_ang(key):
    levels = jnp.sort(jnp.arange(NBLK, dtype=jnp.int32) % (MAXL + 1))
    remaining = levels[BLK_DEV:]
    mixed = remaining[jax.random.permutation(jax.random.fold_in(key, 11), NBLK - BLK_DEV)]
    return jnp.concatenate([jnp.zeros((BLK_DEV,), jnp.int32), mixed]).astype(jnp.int32)


def draw_shell_ang(key, part):
    return shared_ang(key)


def draw_tile_list(key, part):
    angular = shared_ang(key)
    kinds_count = 2 * MAXL + 1
    sixteenth = NTILE // 16
    shares = jnp.array([1, 2, 3, 4, 3, 2, 1], jnp.int32)
    bounds = jnp.cumsum(shares) * sixteenth
    starts = bounds - shares * sixteenth
    position = jnp.arange(NTILE, dtype=jnp.int32)
    kind = jnp.sum((position[:, None] >= bounds[None, :]).astype(jnp.int32), axis=1).astype(jnp.int32)
    device = (position // TILE_DEV).astype(jnp.int32)
    run_start = jnp.maximum(device * TILE_DEV, starts[kind])
    rank_in_run = position - run_start
    orders = []
    sizes = []
    for kind_value in range(kinds_count):
        lowest = max(0, kind_value - MAXL)
        highest = min(MAXL, kind_value)
        eligible = (angular >= lowest) & (angular <= highest)
        ranks = jax.random.permutation(jax.random.fold_in(key, 20 + kind_value), NBLK).astype(jnp.int32)
        scores = jnp.where(eligible, ranks, NBLK + ranks)
        orders.append(jnp.argsort(scores).astype(jnp.int32))
        sizes.append((highest - lowest + 1) * (NBLK // (MAXL + 1)))
    orders = jnp.stack(orders)
    sizes = jnp.array(sizes, jnp.int32)
    offsets = jax.random.randint(jax.random.fold_in(key, 30), (NTILE // TILE_DEV, kinds_count), 0, NBLK).astype(jnp.int32)
    chosen = (offsets[device, kind] + rank_in_run) % sizes[kind]
    bra_block = orders[kind, chosen].astype(jnp.int32)
    lists = []
    for level in range(MAXL + 1):
        ranks = jax.random.permutation(jax.random.fold_in(key, 40 + level), NBLK).astype(jnp.int32)
        scores = jnp.where(angular == level, ranks, NBLK + ranks)
        lists.append(jnp.argsort(scores).astype(jnp.int32))
    lists = jnp.stack(lists)
    needed = (kind - angular[bra_block]).astype(jnp.int32)
    picks = jax.random.randint(jax.random.fold_in(key, 50), (NTILE,), 0, NBLK // (MAXL + 1)).astype(jnp.int32)
    ket_block = lists[needed, picks].astype(jnp.int32)
    return jnp.stack([bra_block, ket_block]).astype(jnp.int32)


def block_scale(stream_key, extent, shards, smallest, high):
    def one(axis_at, shards_of):
        draws = jax.random.uniform(jax.random.fold_in(jax.random.fold_in(stream_key, 6), axis_at), (shards_of,), jnp.float32, smallest / len(shards), high / len(shards))
        return jnp.repeat(jnp.exp(draws), extent[axis_at] // shards_of).reshape((-1,) + (1,) * (len(extent) - axis_at - 1))

    loudness = one(*shards[0])
    for cut in shards[1:]:
        loudness = loudness * one(*cut)
    return loudness


def centred(stream_key, dims, scale, limit, pieces=(), kind=jnp.bfloat16):
    gain = block_scale(stream_key, dims, pieces, -0.22, 0.18) if pieces else 1.0
    entries = jax.random.normal(stream_key, dims, jnp.float32) * scale * gain
    return jnp.minimum(jnp.maximum(entries, -limit), limit).astype(kind)


def setup_inputs(seed: int = 0, part: int = 0) -> dict:
    keys = jax.random.split(jax.random.key(seed), 8)
    own_keys = jax.random.split(jax.random.fold_in(keys[7], part), 8)
    return {
        "coefficient": jnp.clip(jnp.exp(math.log(0.3) - 1.7917595 * jax.random.uniform(own_keys[0], (NPAIR,), jnp.float32) ** block_scale(own_keys[0], (NPAIR,), ((0, 128),), -0.2, 0.2)), 0.05, 0.3),
        "exponent": jnp.clip(jnp.exp(math.log(0.5) - 2.3025851 * jax.random.uniform(own_keys[1], (NPAIR,), jnp.float32) ** block_scale(own_keys[1], (NPAIR,), ((0, 128),), -0.2, 0.2)), 0.05, 0.5),
        "centers": jnp.clip(jax.random.uniform(own_keys[2], (3, NPAIR), jnp.float32, -2.0, 2.0) * block_scale(own_keys[2], (3, NPAIR), ((1, 128),), -0.4, 0.0), -2.0, 2.0),
        "density": centred(own_keys[3], (NPAIR,), 1.0, 6.0, ((0, 128),), jnp.float32),
        "core_fock": centred(own_keys[4], (NPAIR,), 1.0, 6.0, ((0, 128),), jnp.float32),
        "shell_ang": draw_shell_ang(jax.random.fold_in(jax.random.fold_in(keys[7], part), 71), part),
        "tile_list": draw_tile_list(jax.random.fold_in(jax.random.fold_in(keys[7], part), 71), part),
    }


def pair_series(bra_exp, bra_cen, ket_exp, ket_cen, angular):
    distance = jnp.zeros((bra_exp.shape[0], bra_exp.shape[1], ket_exp.shape[1]), jnp.float32)
    for coordinate in range(3):
        offset = bra_cen[coordinate][:, :, None] - ket_cen[coordinate][:, None, :]
        distance = distance + offset * offset
    denominator = bra_exp[:, :, None] + ket_exp[:, None, :] + distance
    ratio = distance / denominator
    series_term = jnp.ones_like(ratio)
    series_sum = jnp.ones_like(ratio)
    for power in range(1, 2 * MAXL + 1):
        series_term = series_term * ratio
        series_sum = series_sum + jnp.where(power <= angular[:, None, None], series_term / (2 * power + 1), 0.0)
    return series_sum * lax.rsqrt(denominator)

def reference(coefficient, exponent, centers, density, core_fock, shell_ang, tile_list):
    coef_blocks = coefficient.reshape(NBLK, PB)
    exp_blocks = exponent.reshape(NBLK, PB)
    cen_blocks = centers.reshape(3, NBLK, PB)
    dens_blocks = density.reshape(NBLK, PB)
    angular = shell_ang[tile_list[0]] + shell_ang[tile_list[1]]
    group_size = 64

    def one_group(packed):
        bra_ids, ket_ids, kinds = packed
        kernel = pair_series(exp_blocks[bra_ids], cen_blocks[:, bra_ids], exp_blocks[ket_ids], cen_blocks[:, ket_ids], kinds)
        value = kernel * coef_blocks[bra_ids][:, :, None] * coef_blocks[ket_ids][:, None, :]
        return jnp.einsum('tij,tj->ti', value, dens_blocks[ket_ids], precision=lax.Precision.HIGHEST)
    partials = lax.map(one_group, (tile_list[0].reshape(-1, group_size), tile_list[1].reshape(-1, group_size), angular.reshape(-1, group_size)))
    coulomb = jnp.zeros((NBLK, PB), jnp.float32).at[tile_list[0]].add(partials.reshape(NTILE, PB))
    return core_fock + coulomb.reshape(NBLK * PB)
```

```python
import functools
from fractions import Fraction
from math import comb

import jax
import jax.numpy as jnp
from jax import lax
from jax.experimental import pallas as pl
from jax.experimental.pallas import tpu as pltpu
from jax.sharding import Mesh
from jax.sharding import PartitionSpec as P

PB = 256
MAXL = 3
NX, NZ, NC = 4, 16, 2
NCHIP = NX * NZ
NDEV = NCHIP * NC
NBLK = 2 * NDEV
GX = ("gx_0", "gx_1", "gx_2")
FRAG_GX = ("frag", "gx_0", "gx_1", "gx_2")
ROWS = 24
BRA_ROW, KET_ROW = 20, 21
MESH = pl.DeviceIdType.MESH
F32, BF16 = jnp.float32, jnp.bfloat16
IO = lambda shape, dim: lax.broadcasted_iota(jnp.int32, shape, dim)


def series_coefficients(kind):
    c = [sum(Fraction((-1) ** n * comb(m, n), 2 * m + 1) for m in range(n, kind + 1)) for n in range(kind + 1)]
    lead = c[kind]
    return float(lead), [float(x / lead) for x in reversed(c[:kind])]


def gather_kernel(coef, expo, cent, dens, tiles, out, chunk, ssem, csem, crecv, zsem, xsem):
    x, z, c = (lax.axis_index(a) for a in GX)
    slot = lambda xx, zz, cc=c: cc * NCHIP + xx * NZ + zz
    zat = lambda d: lax.rem(z + d + NZ, NZ)
    xat = lambda d: lax.rem(x + d + NX, NX)
    own = slot(x, z)

    for r in range(4):
        cut = pl.ds(128 * r, 128)
        for a in range(3):
            chunk[4 * a + r, :] = cent[a, cut]
        chunk[12 + r, :] = expo[cut]
        chunk[16 + r, :] = coef[cut] * dens[cut]
    chunk[BRA_ROW : BRA_ROW + 2, :] = tiles[...].astype(F32)
    chunk[22:24, :] = jnp.zeros((2, 128), F32)
    out[own] = chunk[...]

    barrier = pltpu.get_barrier_semaphore()
    zpeers = [1, -1, 2, -2]
    for d in zpeers:
        pl.semaphore_signal(barrier, inc=1, device_id={"gx_1": zat(d)}, device_id_type=MESH)
    for d in (1, -1):
        pl.semaphore_signal(barrier, inc=1, device_id={"gx_0": xat(d)}, device_id_type=MESH)
    pl.semaphore_signal(barrier, inc=1, device_id={"gx_2": 1 - c}, device_id_type=MESH)
    pl.semaphore_wait(barrier, 7)

    def send(src, at, sem, axis, to):
        pltpu.make_async_remote_copy(
            src_ref=src, dst_ref=out.at[at], send_sem=ssem if axis != "gx_2" else csem, recv_sem=sem,
            device_id={axis: to}, device_id_type=MESH,
        ).start()

    def arrived(at, sem):
        pltpu.make_async_remote_copy(
            src_ref=out.at[at], dst_ref=out.at[at], send_sem=ssem, recv_sem=sem,
            device_id={"gx_2": 1 - c}, device_id_type=MESH,
        ).wait_recv()

    def z_send(src, origin, reach):
        for step in (1, 2):
            d = reach + step * (1 if origin > 0 else -1)
            if -7 <= d <= 8:
                send(src, slot(x, zat(-reach)), zsem.at[d + 7], "gx_1", zat(d - reach))

    def x_send(src, zd):
        at = slot(x, zat(-zd))
        send(src, at, xsem.at[zd + 7, 0], "gx_0", xat(1))
        send(src, at, xsem.at[zd + 7, 1], "gx_0", xat(-1))

    def c_send(src, at):
        send(src, at, crecv, "gx_2", 1 - c)

    def x_take(zd):
        up = slot(xat(-1), zat(-zd))
        down = slot(xat(1), zat(-zd))
        arrived(up, xsem.at[zd + 7, 0])
        if zd % 2 == 0:
            send(out.at[up], up, xsem.at[zd + 7, 2], "gx_0", xat(1))
        c_send(out.at[up], up)
        arrived(down, xsem.at[zd + 7, 1])
        if zd % 2 == 1:
            send(out.at[down], down, xsem.at[zd + 7, 2], "gx_0", xat(-1))
        c_send(out.at[down], down)

    def x_far(zd):
        at = slot(xat(2), zat(-zd))
        arrived(at, xsem.at[zd + 7, 2])
        c_send(out.at[at], at)

    z_send(chunk, 1, 0)
    z_send(chunk, -1, 0)
    x_send(chunk, 0)
    c_send(chunk, own)
    near, far = [0], []
    for rnd in range(1, 5):
        fresh = []
        for d in (2 * rnd, -2 * rnd, 2 * rnd - 1, 1 - 2 * rnd):
            if d < -7:
                continue
            at = slot(x, zat(-d))
            arrived(at, zsem.at[d + 7])
            if d % 2 == 0:
                z_send(out.at[at], d, d)
            x_send(out.at[at], d)
            c_send(out.at[at], at)
            fresh.append(d)
        for d in near:
            x_take(d)
        for d in far:
            x_far(d)
        near, far = fresh, near
    for d in near:
        x_take(d)
    for d in far + near:
        x_far(d)

    plane = out.at[pl.ds((1 - c) * NCHIP, NCHIP)]
    pltpu.make_async_remote_copy(
        src_ref=plane, dst_ref=plane, send_sem=csem, recv_sem=crecv,
        device_id={"gx_2": 1 - c}, device_id_type=MESH,
    ).wait()
    most = out.at[pl.ds(0, NCHIP - 1)]
    pltpu.make_async_remote_copy(
        src_ref=most, dst_ref=most, send_sem=ssem, recv_sem=crecv,
        device_id={"gx_2": 1 - c}, device_id_type=MESH,
    ).wait_send()


def gather_all(coefficient, exponent, centers, density, tile_list):
    return pl.pallas_call(
        gather_kernel,
        out_shape=jax.ShapeDtypeStruct((NDEV, ROWS, 128), F32),
        in_specs=[pl.BlockSpec(memory_space=pltpu.VMEM)] * 5,
        out_specs=pl.BlockSpec(memory_space=pltpu.VMEM),
        scratch_shapes=[
            pltpu.VMEM((ROWS, 128), F32),
            pltpu.SemaphoreType.DMA,
            pltpu.SemaphoreType.DMA,
            pltpu.SemaphoreType.DMA,
            pltpu.SemaphoreType.DMA((16,)),
            pltpu.SemaphoreType.DMA((16, 3)),
        ],
        compiler_params=pltpu.CompilerParams(collective_id=0, has_side_effects=True),
        name="gather_pairs",
    )(coefficient, exponent, centers, density, tile_list)


def split3(v):
    h = v.astype(BF16).astype(F32)
    m = (v - h).astype(BF16).astype(F32)
    return h, m, v - h - m


def ket_rows(v):
    h, m, l = split3(v)
    return jnp.concatenate([h, m, l, h, m, h], axis=0)


def bra_rows(v):
    h, m, l = split3(v)
    return jnp.concatenate([h, h, h, m, m, l], axis=0)


def dot(a, b, dims=((1,), (0,)), **kw):
    return lax.dot_general(a, b, (dims, ((), ())), preferred_element_type=F32, **kw)


NTDIMS = ((1,), (1,))


def tile_kernel(me, ang_s, ang_v, g, coef, core, out, table, feat, ebc, acc, den, lists, slist, sem):
    if me is None:
        x, z, c = (lax.axis_index(a) for a in GX)
        me = (x * NZ + z) * NC + c

    def relayout(p, carry):
        d = lax.rem(p, NCHIP) * NC + p // NCHIP
        base = pl.multiple_of(d * 32, 32)
        cx, cy, cz, e, w = (g[p, 4 * v : 4 * v + 4, :] for v in range(5))
        n = cx * cx + cy * cy + cz * cz + e
        for v, val in enumerate((-2.0 * cx, -2.0 * cy, -2.0 * cz, n, jnp.ones_like(n), e, w, jnp.zeros_like(n))):
            table[pl.ds(base + v, 4, stride=8), :] = val
        return carry

    lax.fori_loop(0, NDEV, relayout, 0, unroll=4)

    bra = g[:, BRA_ROW, :].astype(jnp.int32) - 2 * me
    ket = g[:, KET_ROW, :].astype(jnp.int32)
    mine = (bra >= 0) & (bra < 2)
    high = jnp.where(mine, bra * 16 + ket // 16, -1)
    low = ket & 15
    count = jnp.zeros((32, 16), F32)
    step = 16
    for r in range(0, NDEV, step):
        a = [(IO((32, 128), 0) == high[r + k : r + k + 1, :]).astype(F32).astype(BF16) for k in range(step)]
        b = [(IO((16, 128), 0) == low[r + k : r + k + 1, :]).astype(F32).astype(BF16) for k in range(step)]
        count = count + dot(jnp.concatenate(a, axis=1), jnp.concatenate(b, axis=1), NTDIMS)
    spread = (IO((16, 256), 1) % 16 == IO((16, 256), 0)).astype(F32)
    wide = dot(count, spread, precision=lax.Precision.HIGHEST)
    wide = jnp.where(IO((32, 256), 0) % 16 == IO((32, 256), 1) // 16, wide, 0.0)
    mult = [jnp.sum(wide[16 * b : 16 * b + 16], axis=0, keepdims=True) for b in range(2)]

    ang_row = ang_v[...].reshape(1, NBLK)
    row_i, col_i = IO((NBLK, NBLK), 0), IO((NBLK, NBLK), 1)
    key_row = ang_row * NBLK + IO((1, NBLK), 1)
    key_col = jnp.sum(jnp.where(row_i == col_i, key_row.astype(F32), 0.0), axis=1, keepdims=True).astype(jnp.int32)
    before = (key_col < key_row).astype(F32).astype(BF16)
    level = (key_col < IO((NBLK, 128), 1) * NBLK).astype(F32).astype(BF16)
    valid = [(m > 0.0).astype(F32) for m in mult]
    valid8 = jnp.concatenate(valid + [jnp.zeros((6, NBLK), F32)], axis=0).astype(BF16)
    rank = dot(valid8, before)
    starts = dot(valid8, level)
    ids = IO((1, NBLK), 1).astype(F32)
    for b in range(2):
        where_b = jnp.where(valid[b] > 0.0, rank[b : b + 1].astype(jnp.int32), -1)
        onehot = (where_b == row_i).astype(F32).astype(BF16)
        m_hi = jnp.floor(mult[b] * (1.0 / 16.0))
        src = jnp.concatenate([ids, mult[b] - 16.0 * m_hi, m_hi, jnp.zeros((5, NBLK), F32)], axis=0).astype(BF16)
        got = dot(src, onehot, NTDIMS)
        lists[2 * b : 2 * b + 1, :] = got[0:1].astype(jnp.int32)
        lists[2 * b + 1 : 2 * b + 2, :] = (got[1:2] + 16.0 * got[2:3]).astype(jnp.int32)
        lists[4 + b : 5 + b, 0:128] = starts[b : b + 1].astype(jnp.int32)
    to_smem = pltpu.make_async_copy(lists, slist, sem)
    to_smem.start()

    for q in range(4):
        grp = table[pl.ds(pl.multiple_of(me * 32 + 8 * q, 8), 8), :]
        v = grp[0:3] * -0.5
        v = jnp.concatenate([v, jnp.ones((1, 128), F32), grp[3:4], jnp.zeros((3, 128), F32)], axis=0)
        full = jnp.concatenate([bra_rows(v), grp, jnp.zeros((72, 128), F32)], axis=0).T
        feat[128 * q : 128 * q + 128, :] = full[:, 0:48].astype(BF16)
        ebc[128 * q : 128 * q + 128, :] = jnp.broadcast_to(full[:, 53:54], (128, 128))
    acc[...] = jnp.zeros_like(acc)
    to_smem.wait()

    CH = 64

    def ket_side(b, p):
        k = slist[2 * b, p]
        rows = [table[pl.ds(pl.multiple_of(k * 16 + 8 * h, 8), 8), :] for h in range(2)]
        return jnp.concatenate([ket_rows(v) for v in rows], axis=1).astype(BF16)

    for b in range(2):
        total = slist[4 + b, 4]

        @pl.when(total > 0)
        def _():
            rhs = ket_side(b, 0)
            den[0] = dot(feat[256 * b : 256 * b + 256, :], rhs)

            def run(kind, lo, hi):
                lead, lower = series_coefficients(kind)

                def body(p, carry):
                    now = lax.rem(p, 2)
                    rhs = ket_side(b, jnp.minimum(p + 1, NBLK - 1))
                    k = slist[2 * b, p]
                    times = slist[2 * b + 1, p].astype(F32) * lead
                    er, wr = [], []
                    for h in range(2):
                        at = k * 16 + 8 * h
                        er.append(jnp.broadcast_to(table[pl.ds(at + 5, 1), :], (8, 128)))
                        wr.append(jnp.broadcast_to(table[pl.ds(at + 6, 1), :] * times, (8, 128)))
                    for i in range(0, PB, CH):
                        cut = pl.ds(256 * b + i, CH)
                        nxt = dot(feat[cut, :], rhs)
                        sums = None
                        for h in range(2):
                            d = den[now, i : i + CH, 128 * h : 128 * h + 128].reshape(CH // 8, 8, 128)
                            r = lax.rsqrt(d)
                            v = r * wr[h]
                            if kind:
                                t = (ebc[cut, :].reshape(CH // 8, 8, 128) + er[h]) * (r * r)
                                poly = t + lower[0]
                                for coefficient in lower[1:]:
                                    poly = poly * t + coefficient
                                v = v * poly
                            sums = v if sums is None else sums + v
                        acc[cut, :] += sums.reshape(CH, 128)
                        den[1 - now, i : i + CH, :] = nxt
                    return carry

                lax.fori_loop(lo, hi, body, 0)

            ang_b = ang_s[2 * me + b]
            for l in range(MAXL + 1):
                lo, hi = slist[4 + b, l], slist[4 + b, l + 1]
                lax.switch(ang_b + l - l, [functools.partial(run, a + l, lo, hi) for a in range(MAXL + 1)])

    for q in range(4):
        total = jnp.sum(acc[128 * q : 128 * q + 128, :].T, axis=0)
        cut = pl.ds(128 * q, 128)
        out[cut] = core[cut] + coef[cut] * total


def tile_sums(gathered, shell_ang, coefficient, core_fock, me=None, interpret=False):
    vm = pl.BlockSpec(memory_space=pltpu.VMEM)
    return pl.pallas_call(
        functools.partial(tile_kernel, me),
        out_shape=jax.ShapeDtypeStruct((2 * PB,), F32),
        in_specs=[pl.BlockSpec(memory_space=pltpu.SMEM), vm, vm, vm, vm],
        out_specs=vm,
        scratch_shapes=[
            pltpu.VMEM((NBLK * 16, 128), F32),
            pltpu.VMEM((2 * PB, 48), BF16),
            pltpu.VMEM((2 * PB, 128), F32),
            pltpu.VMEM((2 * PB, 128), F32),
            pltpu.VMEM((2, PB, PB), F32),
            pltpu.VMEM((8, NBLK), jnp.int32),
            pltpu.SMEM((8, NBLK), jnp.int32),
            pltpu.SemaphoreType.DMA,
        ],
        name="tile_sums",
        interpret=interpret,
    )(shell_ang, shell_ang, gathered, coefficient, core_fock)


def shards(coefficient, exponent, centers, density, core_fock, shell_ang, tile_list):
    gathered = gather_all(coefficient, exponent, centers, density, tile_list)
    return tile_sums(gathered, shell_ang, coefficient, core_fock)


def solution(mesh):
    finer = Mesh(mesh.devices.reshape(mesh.shape["frag"], NX, NZ, NC), FRAG_GX)
    return jax.shard_map(
        shards,
        mesh=finer,
        in_specs=(
            P(FRAG_GX),
            P(FRAG_GX),
            P(None, FRAG_GX),
            P(FRAG_GX),
            P(FRAG_GX),
            P("frag"),
            P(None, FRAG_GX),
        ),
        out_specs=P(FRAG_GX),
        check_vma=False,
    )
```
